16 devices in a mesh: dp: 4 (over y, z, core), tp: 4 (over x).
Axes of the slice: x: 4, y: 2, z: 1, core: 2. Of those that a mesh axis runs over, the one named last changes fastest.
The devices are a block of a 4x4x8 slice.
Arguments:
- x: bfloat16 [8192, 2048], P('dp'), parts along dimension 0
- w_gate: bfloat16 [2048, 8192], P(None, 'tp')
- w_up: bfloat16 [2048, 8192], P(None, 'tp')
- w_down: bfloat16 [8192, 2048], P('tp')
Outputs:
- output: bfloat16 [8192, 2048], P('dp'), parts along dimension 0
There are 4 independent parts. The reference program is written for one: setup_inputs(seed, part) draws one part's arguments, and reference() takes and returns one part's arrays. A program takes and returns all parts, laid end to end along the dimension named above; an argument that names none is the same for every part.
All inputs are finite; a program needn't handle non-finite values.
Results may differ from the reference program's by a relative error of at most 0.016.
Values are sent between devices in bfloat16 or wider.
A program may use at most 768 MiB of HBM per device.

```python
import jax
import jax.numpy as jnp

ROWS = 2048
D = 2048
FF = 8192


def setup_inputs(seed: int = 0, part: int = 0) -> dict:
    kx, kg, ku, kd = jax.random.split(jax.random.key(seed), 4)
    drawn = {
        "x": jax.random.normal(jax.random.fold_in(kx, part), (ROWS, D), jnp.float32),
        "w_gate": jax.random.normal(kg, (D, FF), jnp.float32) * D**-0.5,
        "w_up": jax.random.normal(ku, (D, FF), jnp.float32) * D**-0.5,
        "w_down": jax.random.normal(kd, (FF, D), jnp.float32) * FF**-0.5,
    }
    return {k: v.astype(jnp.bfloat16) for k, v in drawn.items()}


def reference(x, w_gate, w_up, w_down):
    gate = jnp.dot(x, w_gate, preferred_element_type=jnp.float32)
    up = jnp.dot(x, w_up, preferred_element_type=jnp.float32)
    hidden = (jax.nn.silu(gate) * up).astype(jnp.bfloat16)
    return jnp.dot(hidden, w_down, preferred_element_type=jnp.float32).astype(jnp.bfloat16)
```

```python
import functools

import jax
import jax.numpy as jnp
from jax import lax
from jax.experimental import pallas as pl
from jax.experimental.pallas import tpu as pltpu
from jax.sharding import PartitionSpec as P

COLS = 512


def kernel(x_ref, wg_ref, wu_ref, wd_ref, y_ref, xbuf, wg, wu, wd, hid, sbuf, rbuf, own, fin,
           x_sem, w_sem, d_sem, send_sem, recv_sem, ag_send, ag_recv, loc_sem):
    n = 4
    me = lax.axis_index("tp")
    right, left = lax.rem(me + 1, n), lax.rem(me + n - 1, n)
    rows, depth = x_ref.shape
    width = wg_ref.shape[1]
    chunk = rows // n
    half = chunk // 2
    sub = half // 2
    steps = width // COLS
    dsteps = wd_ref.shape[1] // COLS

    def row_of(owner, part, s):
        return pl.multiple_of(lax.rem(owner, n) * chunk + part * half + s * sub, sub)

    def x_copies(p):
        kind, s, slot = p // 2, lax.rem(p, 2), lax.rem(p, 2)
        r = row_of(me + (4 - kind) // 2, lax.rem(kind + 1, 2), s)
        l = row_of(me + 2 + (kind + 1) // 2, lax.rem(kind, 2), s)
        return (
            pltpu.make_async_copy(x_ref.at[pl.ds(r, sub)], xbuf.at[slot, pl.ds(0, sub)], x_sem.at[slot, 0]),
            pltpu.make_async_copy(x_ref.at[pl.ds(l, sub)], xbuf.at[slot, pl.ds(sub, sub)], x_sem.at[slot, 1]),
        )

    def w_copies(c):
        cols = pl.ds(pl.multiple_of(c * COLS, COLS), COLS)
        return (
            pltpu.make_async_copy(wg_ref.at[:, cols], wg.at[:, cols], w_sem.at[c, 0]),
            pltpu.make_async_copy(wu_ref.at[:, cols], wu.at[:, cols], w_sem.at[c, 1]),
        )

    def d_copy(c):
        cols = pl.ds(pl.multiple_of(c * COLS, COLS), COLS)
        return pltpu.make_async_copy(wd_ref.at[:, cols], wd.at[:, cols], d_sem.at[c])

    def remote(src, dst, ssem, rsem, to):
        return pltpu.make_async_remote_copy(
            src_ref=src, dst_ref=dst, send_sem=ssem, recv_sem=rsem,
            device_id={"tp": to}, device_id_type=pl.DeviceIdType.MESH)

    def rs_copies(kind, s):
        p = 2 * kind + s
        lo, hi = pl.ds(0, sub), pl.ds(sub, sub)
        dr, dl = (hi, lo) if kind == 2 else (lo, hi)
        return (
            remote(sbuf.at[p, lo], rbuf.at[kind, s, dr], send_sem.at[p, 0], recv_sem.at[p, 0], right),
            remote(sbuf.at[p, hi], rbuf.at[kind, s, dl], send_sem.at[p, 1], recv_sem.at[p, 1], left),
        )

    for c in x_copies(0):
        c.start()
    for c in range(steps):
        for w in w_copies(c):
            w.start()
    for c in range(dsteps):
        d_copy(c).start()

    barrier = pltpu.get_barrier_semaphore()
    for to in (left, right):
        pl.semaphore_signal(barrier, inc=1, device_id={"tp": to}, device_id_type=pl.DeviceIdType.MESH)
    pl.semaphore_wait(barrier, 2)

    def run_pass(kind, s, first):
        p = 2 * kind + s
        slot = s
        for c in x_copies(p):
            c.wait()

        @pl.when(p < 7)
        def _():
            for c in x_copies(p + 1):
                c.start()

        def up_step(c, _):
            @pl.when(first)
            def _():
                for w in w_copies(c):
                    w.wait()
            cols = pl.ds(pl.multiple_of(c * COLS, COLS), COLS)
            xv = xbuf[slot]
            g = jnp.dot(xv, wg[:, cols], preferred_element_type=jnp.float32)
            u = jnp.dot(xv, wu[:, cols], preferred_element_type=jnp.float32)
            hid[:, cols] = (jax.nn.silu(g) * u).astype(jnp.bfloat16)
            return 0

        lax.fori_loop(0, steps, up_step, 0)

        if kind >= 2:
            for c in rs_copies(kind - 2, s):
                c.wait_recv()

        def down_step(c, _):
            @pl.when(first)
            def _():
                d_copy(c).wait()
            cols = pl.ds(pl.multiple_of(c * COLS, COLS), COLS)
            t = jnp.dot(hid[...], wd[:, cols], preferred_element_type=jnp.float32)
            if kind >= 2:
                t = t + rbuf[kind - 2, s, :, cols].astype(jnp.float32)
            if kind < 3:
                sbuf[p, :, cols] = t.astype(jnp.bfloat16)
            else:
                own[s, :, cols] = t
            return 0

        lax.fori_loop(0, dsteps, down_step, 0)
        if kind < 3:
            for c in rs_copies(kind, s):
                c.start()

    for kind in range(4):
        def body(s, _, kind=kind):
            run_pass(kind, s, (s == 0) if kind == 0 else False)
            return 0
        lax.fori_loop(0, 2, body, 0)

    def ag(src, owner, part, s, d, slot):
        at = pl.ds(row_of(owner, part, s), sub)
        return remote(src, y_ref.at[at], ag_send.at[s, d, slot], ag_recv.at[s, d, slot], (right, left)[d])

    def finished(part, s):
        return fin.at[s, pl.ds(part * sub, sub)]

    def local(part, s):
        return pltpu.make_async_copy(finished(part, s), y_ref.at[pl.ds(row_of(me, part, s), sub)], loc_sem.at[s, part])

    for s in range(2):
        for c in rs_copies(2, s):
            c.wait_recv()
        fin[s] = (own[s] + rbuf[2, s].astype(jnp.float32)).astype(jnp.bfloat16)
        for part in range(2):
            for d in range(2):
                q = part if d == 0 else 1 - part
                ag(finished(q, s), me, q, s, d, q).start()
        for part in range(2):
            local(part, s).start()

    def forward(s, d):
        owner = left if d == 0 else right
        at = pl.ds(row_of(owner, d, s), sub)
        return ag(y_ref.at[at], owner, d, s, d, 2)

    for s in range(2):
        for d in range(2):
            ag(finished(d, s), me, d, s, d, d).wait_recv()
            forward(s, d).start()
    for s in range(2):
        for d in range(2):
            ag(finished(1 - d, s), me, 1 - d, s, d, 1 - d).wait_recv()
            forward(s, d).wait_recv()
    for s in range(2):
        for part in range(2):
            local(part, s).wait()
        for kind in range(3):
            for c in rs_copies(kind, s):
                c.wait_send()
        for d in range(2):
            for q in range(2):
                ag(finished(q, s), me, q, s, d, q).wait_send()
            forward(s, d).wait_send()


def solution(mesh):
    n = mesh.shape["tp"]
    assert n == 4

    def step(x, w_gate, w_up, w_down):
        rows, depth = x.shape
        width, out = w_down.shape
        block = rows // n // 2
        bf16, f32 = jnp.bfloat16, jnp.float32
        any_ = pl.BlockSpec(memory_space=pl.ANY)
        dma = pltpu.SemaphoreType.DMA
        return pl.pallas_call(
            kernel,
            out_shape=jax.ShapeDtypeStruct((rows, out), bf16),
            in_specs=[any_] * 4,
            out_specs=any_,
            scratch_shapes=[
                pltpu.VMEM((2, block, depth), bf16),
                pltpu.VMEM((depth, width), bf16),
                pltpu.VMEM((depth, width), bf16),
                pltpu.VMEM((width, out), bf16),
                pltpu.VMEM((block, width), bf16),
                pltpu.VMEM((6, block, out), bf16),
                pltpu.VMEM((3, 2, block, out), bf16),
                pltpu.VMEM((2, block, out), f32),
                pltpu.VMEM((2, block, out), bf16),
                dma((2, 2)),
                dma((width // COLS, 2)),
                dma((out // COLS,)),
                dma((6, 2)),
                dma((6, 2)),
                dma((2, 2, 3)),
                dma((2, 2, 3)),
                dma((2, 2)),
            ],
            compiler_params=pltpu.CompilerParams(
                collective_id=0, has_side_effects=True, vmem_limit_bytes=56 * 2**20
            ),
            cost_estimate=pl.CostEstimate(
                flops=6 * rows * depth * width, bytes_accessed=2 * (2 * rows * depth + 3 * depth * width), transcendentals=rows * width),
            name="mlp_block",
        )(x, w_gate, w_up, w_down)

    return jax.shard_map(
        step,
        mesh=mesh,
        in_specs=(P("dp", None), P(None, "tp"), P(None, "tp"), P("tp", None)),
        out_specs=P("dp", None),
        check_vma=False,
    )
```

```python
import functools

import jax
import jax.numpy as jnp
from jax import lax
from jax.experimental import pallas as pl
from jax.experimental.pallas import tpu as pltpu
from jax.sharding import PartitionSpec as P

COLS = 512
LOAD = 256
AHEAD = 3


def kernel(x_ref, wg_ref, wu_ref, wd_ref, y_ref, xbuf, wg, wu, wd, hid, sbuf, rbuf, own, fin,
           x_sem, w_sem, d_sem, send_sem, recv_sem, ag_send, ag_recv, loc_sem, first_send, first_recv):
    n = 4
    me = lax.axis_index("tp")
    right, left = lax.rem(me + 1, n), lax.rem(me + n - 1, n)
    rows, depth = x_ref.shape
    width = wg_ref.shape[1]
    chunk = rows // n
    half = chunk // 2
    sub = half // 2
    steps, dsteps = width // COLS, wd_ref.shape[1] // COLS
    loads, dloads = width // LOAD, wd_ref.shape[1] // LOAD

    def row_of(owner, part, s):
        return pl.multiple_of(lax.rem(owner, n) * chunk + part * half + s * sub, sub)

    def x_copies(p):
        kind, s, slot = p // 2, lax.rem(p, 2), lax.rem(p, 2)
        r = row_of(me + (4 - kind) // 2, lax.rem(kind + 1, 2), s)
        l = row_of(me + 2 + (kind + 1) // 2, lax.rem(kind, 2), s)
        return (
            pltpu.make_async_copy(x_ref.at[pl.ds(r, sub)], xbuf.at[slot, pl.ds(0, sub)], x_sem.at[slot, 0]),
            pltpu.make_async_copy(x_ref.at[pl.ds(l, sub)], xbuf.at[slot, pl.ds(sub, sub)], x_sem.at[slot, 1]),
        )

    def load_cols(c):
        return pl.ds(pl.multiple_of(c * LOAD, LOAD), LOAD)

    def w_copies(c):
        cols = load_cols(c)
        return (
            pltpu.make_async_copy(wg_ref.at[:, cols], wg.at[:, cols], w_sem.at[c, 0]),
            pltpu.make_async_copy(wu_ref.at[:, cols], wu.at[:, cols], w_sem.at[c, 1]),
        )

    def d_copy(c):
        cols = load_cols(c)
        return pltpu.make_async_copy(wd_ref.at[:, cols], wd.at[:, cols], d_sem.at[c])

    def remote(src, dst, ssem, rsem, to):
        return pltpu.make_async_remote_copy(
            src_ref=src, dst_ref=dst, send_sem=ssem, recv_sem=rsem,
            device_id={"tp": to}, device_id_type=pl.DeviceIdType.MESH)

    lo, hi = pl.ds(0, sub), pl.ds(sub, sub)

    def rs_copies(kind, s):
        p = 2 * kind + s
        dr, dl = (hi, lo) if kind == 2 else (lo, hi)
        return (
            remote(sbuf.at[p, lo], rbuf.at[kind, s, dr], send_sem.at[p, 0], recv_sem.at[p, 0], right),
            remote(sbuf.at[p, hi], rbuf.at[kind, s, dl], send_sem.at[p, 1], recv_sem.at[p, 1], left),
        )

    def first_copies(c):
        cols = load_cols(c)
        return (
            remote(sbuf.at[0, lo, cols], rbuf.at[0, 0, lo, cols], first_send.at[c, 0], first_recv.at[c, 0], right),
            remote(sbuf.at[0, hi, cols], rbuf.at[0, 0, hi, cols], first_send.at[c, 1], first_recv.at[c, 1], left),
        )

    def gate_up(slot, cols):
        xv = xbuf[slot]
        g = jnp.dot(xv, wg[:, cols], preferred_element_type=jnp.float32)
        u = jnp.dot(xv, wu[:, cols], preferred_element_type=jnp.float32)
        hid[:, cols] = (jax.nn.silu(g) * u).astype(jnp.bfloat16)

    for c in x_copies(0):
        c.start()
    for c in range(AHEAD):
        for w in w_copies(c):
            w.start()

    def first_up(c, _):
        for w in w_copies(c):
            w.wait()

        @pl.when(c < loads - AHEAD)
        def _():
            for w in w_copies(c + AHEAD):
                w.start()

        @pl.when(c >= loads - AHEAD)
        def _():
            d_copy(c - (loads - AHEAD)).start()

        gate_up(0, load_cols(c))
        return 0

    def first_down(c, _):
        d_copy(c).wait()

        @pl.when(c < dloads - AHEAD)
        def _():
            d_copy(c + AHEAD).start()

        cols = load_cols(c)
        t = jnp.dot(hid[...], wd[:, cols], preferred_element_type=jnp.float32)
        sbuf[0, :, cols] = t.astype(jnp.bfloat16)
        for r in first_copies(c):
            r.start()
        return 0

    for c in x_copies(0):
        c.wait()
    lax.fori_loop(0, loads, first_up, 0)
    for c in x_copies(1):
        c.start()
    barrier = pltpu.get_barrier_semaphore()
    for to in (left, right):
        pl.semaphore_signal(barrier, inc=1, device_id={"tp": to}, device_id_type=pl.DeviceIdType.MESH)
    pl.semaphore_wait(barrier, 2)
    lax.fori_loop(0, dloads, first_down, 0)

    def recv_wait(kind, s):
        if kind == 0:
            @pl.when(s == 0)
            def _():
                def one(c, _):
                    for r in first_copies(c):
                        r.wait_recv()
                    return 0
                lax.fori_loop(0, dloads, one, 0)

            @pl.when(s > 0)
            def _():
                for c in rs_copies(0, s):
                    c.wait_recv()
        else:
            for c in rs_copies(kind, s):
                c.wait_recv()

    def run_pass(kind, s):
        p = 2 * kind + s
        for c in x_copies(p):
            c.wait()

        @pl.when(p < 7)
        def _():
            for c in x_copies(p + 1):
                c.start()

        def cols_of(c):
            return pl.ds(pl.multiple_of(c * COLS, COLS), COLS)

        def up_step(c, _):
            gate_up(s, cols_of(c))
            return 0

        lax.fori_loop(0, steps, up_step, 0)

        if kind >= 2:
            recv_wait(kind - 2, s)

        def down_step(c, _):
            cols = cols_of(c)
            t = jnp.dot(hid[...], wd[:, cols], preferred_element_type=jnp.float32)
            if kind >= 2:
                t = t + rbuf[kind - 2, s, :, cols].astype(jnp.float32)
            if kind < 3:
                sbuf[p, :, cols] = t.astype(jnp.bfloat16)
            else:
                own[s, :, cols] = t
            return 0

        lax.fori_loop(0, dsteps, down_step, 0)
        if kind < 3:
            for c in rs_copies(kind, s):
                c.start()

    for kind in range(4):
        def body(s, _, kind=kind):
            run_pass(kind, s)
            return 0
        lax.fori_loop(1 if kind == 0 else 0, 2, body, 0)

    def ag(src, owner, part, s, d, slot):
        at = pl.ds(row_of(owner, part, s), sub)
        return remote(src, y_ref.at[at], ag_send.at[s, d, slot], ag_recv.at[s, d, slot], (right, left)[d])

    def finished(part, s):
        return fin.at[s, pl.ds(part * sub, sub)]

    def local(part, s):
        return pltpu.make_async_copy(finished(part, s), y_ref.at[pl.ds(row_of(me, part, s), sub)], loc_sem.at[s, part])

    for s in range(2):
        for c in rs_copies(2, s):
            c.wait_recv()
        fin[s] = (own[s] + rbuf[2, s].astype(jnp.float32)).astype(jnp.bfloat16)
        for part in range(2):
            for d in range(2):
                q = part if d == 0 else 1 - part
                ag(finished(q, s), me, q, s, d, q).start()
        for part in range(2):
            local(part, s).start()

    def forward(s, d):
        owner = left if d == 0 else right
        at = pl.ds(row_of(owner, d, s), sub)
        return ag(y_ref.at[at], owner, d, s, d, 2)

    for s in range(2):
        for d in range(2):
            ag(finished(d, s), me, d, s, d, d).wait_recv()
            forward(s, d).start()
    for s in range(2):
        for d in range(2):
            ag(finished(1 - d, s), me, 1 - d, s, d, 1 - d).wait_recv()
            forward(s, d).wait_recv()
    def first_sent(c, _):
        for r in first_copies(c):
            r.wait_send()
        return 0

    lax.fori_loop(0, dloads, first_sent, 0)
    for s in range(2):
        for part in range(2):
            local(part, s).wait()
        for kind in range(3):
            if kind + s > 0:
                for c in rs_copies(kind, s):
                    c.wait_send()
        for d in range(2):
            for q in range(2):
                ag(finished(q, s), me, q, s, d, q).wait_send()
            forward(s, d).wait_send()


def solution(mesh):
    n = mesh.shape["tp"]
    assert n == 4

    def step(x, w_gate, w_up, w_down):
        rows, depth = x.shape
        width, out = w_down.shape
        block = rows // n // 2
        bf16, f32 = jnp.bfloat16, jnp.float32
        any_ = pl.BlockSpec(memory_space=pl.ANY)
        dma = pltpu.SemaphoreType.DMA
        return pl.pallas_call(
            kernel,
            out_shape=pltpu.VMEM((rows, out), bf16),
            in_specs=[any_] * 4,
            out_specs=any_,
            scratch_shapes=[
                pltpu.VMEM((2, block, depth), bf16),
                pltpu.VMEM((depth, width), bf16),
                pltpu.VMEM((depth, width), bf16),
                pltpu.VMEM((width, out), bf16),
                pltpu.VMEM((block, width), bf16),
                pltpu.VMEM((6, block, out), bf16),
                pltpu.VMEM((3, 2, block, out), bf16),
                pltpu.VMEM((2, block, out), f32),
                pltpu.VMEM((2, block, out), bf16),
                dma((2, 2)),
                dma((width // LOAD, 2)),
                dma((out // LOAD,)),
                dma((6, 2)),
                dma((6, 2)),
                dma((2, 2, 3)),
                dma((2, 2, 3)),
                dma((2, 2)),
                dma((out // LOAD, 2)),
                dma((out // LOAD, 2)),
            ],
            compiler_params=pltpu.CompilerParams(
                collective_id=0, has_side_effects=True, vmem_limit_bytes=52 * 2**20
            ),
            cost_estimate=pl.CostEstimate(
                flops=6 * rows * depth * width, bytes_accessed=2 * (2 * rows * depth + 3 * depth * width), transcendentals=rows * width),
            name="mlp_block",
        )(x, w_gate, w_up, w_down)

    return jax.shard_map(
        step,
        mesh=mesh,
        in_specs=(P("dp", None), P(None, "tp"), P(None, "tp"), P("tp", None)),
        out_specs=P("dp", None),
        check_vma=False,
    )
```

```python
import jax
import jax.numpy as jnp
from jax import lax
from jax.experimental import pallas as pl
from jax.experimental.pallas import tpu as pltpu
from jax.sharding import PartitionSpec as P

COLS = 512
UP = (512, 512, 512, 512)
DOWN = (512, 512, 512, 512)
AHEAD = 3
MINI = 4
MINI_SEND = 1024


def kernel(x_ref, wg_ref, wu_ref, wd_ref, y_ref, xmini, xbuf, wg, wu, wd, hid, sbuf, rbuf, own,
           xm_sem, x_sem, w_sem, d_sem, ms_sem, mr_sem, send_sem, recv_sem, ag_send, ag_recv):
    n = 4
    me = lax.axis_index("tp")
    right, left = lax.rem(me + 1, n), lax.rem(me + n - 1, n)
    rows = x_ref.shape[0]
    width, out = wd_ref.shape
    chunk = rows // n
    half = chunk // 2
    sub = half // 2
    mini = half // MINI

    def row_of(owner, part, at, size):
        return pl.ds(pl.multiple_of(lax.rem(owner, n) * chunk + part * half + at, size), size)

    def remote(src, dst, ssem, rsem, to):
        return pltpu.make_async_remote_copy(
            src_ref=src, dst_ref=dst, send_sem=ssem, recv_sem=rsem,
            device_id={"tp": to}, device_id_type=pl.DeviceIdType.MESH)

    def x_pair(kind, at, size, buf, sem):
        r = row_of(me + (4 - kind) // 2, lax.rem(kind + 1, 2), at, size)
        l = row_of(me + 2 + (kind + 1) // 2, lax.rem(kind, 2), at, size)
        return (
            pltpu.make_async_copy(x_ref.at[r], buf.at[pl.ds(0, size)], sem.at[0]),
            pltpu.make_async_copy(x_ref.at[l], buf.at[pl.ds(size, size)], sem.at[1]),
        )

    def x_mini(q):
        slot = lax.rem(q, 2)
        return x_pair(0, q * mini, mini, xmini.at[slot], xm_sem.at[slot])

    def x_pass(p):
        slot = lax.rem(p, 2)
        return x_pair(p // 2, slot * sub, sub, xbuf.at[slot], x_sem.at[slot])

    def w_copies(c):
        cols = pl.ds(sum(UP[:c]), UP[c])
        return (
            pltpu.make_async_copy(wg_ref.at[:, cols], wg.at[:, cols], w_sem.at[c, 0]),
            pltpu.make_async_copy(wu_ref.at[:, cols], wu.at[:, cols], w_sem.at[c, 1]),
        )

    def d_copy(c):
        cols = pl.ds(sum(DOWN[:c]), DOWN[c])
        return pltpu.make_async_copy(wd_ref.at[:, cols], wd.at[:, cols], d_sem.at[c])

    def mini_rows(q, d):
        return pl.ds(pl.multiple_of(lax.rem(q, 2) * mini + d * sub, mini), mini)

    def mini_copies(q, cols=slice(None)):
        s = q // 2
        return tuple(
            remote(sbuf.at[s, mini_rows(q, d), cols], rbuf.at[0, s, mini_rows(q, d), cols],
                   ms_sem.at[q, d], mr_sem.at[q, d], (right, left)[d])
            for d in range(2))

    def pass_copies(kind, s, cols=slice(None)):
        p = 2 * kind + s
        return tuple(
            remote(sbuf.at[p, pl.ds(d * sub, sub), cols],
                   rbuf.at[kind, s, pl.ds((1 - d if kind == 2 else d) * sub, sub), cols],
                   send_sem.at[p, d], recv_sem.at[p, d], (right, left)[d])
            for d in range(2))

    def gate_up(xv, cols):
        m = xv.shape[0]
        g = jnp.dot(xv, wg[:, cols], preferred_element_type=jnp.float32)
        u = jnp.dot(xv, wu[:, cols], preferred_element_type=jnp.float32)
        hid[pl.ds(0, m), cols] = (jax.nn.silu(g) * u).astype(jnp.bfloat16)

    def down(m, cols):
        return jnp.dot(hid[pl.ds(0, m)], wd[:, cols], preferred_element_type=jnp.float32)

    def step_cols(c):
        return pl.ds(pl.multiple_of(c * COLS, COLS), COLS)

    barrier = pltpu.get_barrier_semaphore()
    for to in (left, right):
        pl.semaphore_signal(barrier, inc=1, device_id={"tp": to}, device_id_type=pl.DeviceIdType.MESH)

    for c in x_mini(0):
        c.start()
    weights = [w_copies(c) for c in range(len(UP))] + [(d_copy(c),) for c in range(len(DOWN))]

    def load(i):
        if i < len(weights):
            for w in weights[i]:
                w.start()

    for i in range(AHEAD):
        load(i)
    for c in x_mini(1):
        c.start()

    def store_mini(q, cols):
        t = down(2 * mini, cols).astype(jnp.bfloat16)
        for d in range(2):
            sbuf[q // 2, mini_rows(q, d), cols] = t[d * mini:(d + 1) * mini]

    for c in x_mini(0):
        c.wait()
    for c in range(len(UP)):
        for w in w_copies(c):
            w.wait()
        load(c + AHEAD)
        gate_up(xmini[0], pl.ds(sum(UP[:c]), UP[c]))
    pl.semaphore_wait(barrier, 2)
    for c in range(len(DOWN)):
        d_copy(c).wait()
        load(len(UP) + c + AHEAD)
        cols = pl.ds(sum(DOWN[:c]), DOWN[c])
        store_mini(0, cols)
        for r in mini_copies(0, cols):
            r.start()

    def mini_pass(q, _):
        for c in x_mini(q):
            c.wait()

        @pl.when(q < MINI - 1)
        def _():
            for c in x_mini(q + 1):
                c.start()

        @pl.when(q == MINI - 1)
        def _():
            for c in x_pass(2):
                c.start()

        slot = lax.rem(q, 2)

        def up_step(c, _):
            gate_up(xmini[slot], step_cols(c))
            return 0

        lax.fori_loop(0, width // COLS, up_step, 0)

        def down_steps(b, _):
            def down_step(c, _):
                store_mini(q, step_cols(c))
                return 0

            each = MINI_SEND // COLS
            lax.fori_loop(b * each, (b + 1) * each, down_step, 0)
            for r in mini_copies(q, pl.ds(pl.multiple_of(b * MINI_SEND, MINI_SEND), MINI_SEND)):
                r.start()
            return 0

        lax.fori_loop(0, out // MINI_SEND, down_steps, 0)
        return 0

    lax.fori_loop(1, MINI, mini_pass, 0)

    def run_pass(kind, s):
        p = 2 * kind + s
        for c in x_pass(p):
            c.wait()

        @pl.when(p < 7)
        def _():
            for c in x_pass(p + 1):
                c.start()

        def up_step(c, _):
            gate_up(xbuf[s], step_cols(c))
            return 0

        lax.fori_loop(0, width // COLS, up_step, 0)

        if kind == 2:
            for j in range(MINI // 2):
                for c in mini_copies(s * (MINI // 2) + j):
                    c.wait_recv()
        if kind == 3:
            for c in pass_copies(1, s):
                c.wait_recv()

        def down_step(c, _):
            cols = step_cols(c)
            t = down(2 * sub, cols)
            if kind >= 2:
                t = t + rbuf[kind - 2, s, :, cols].astype(jnp.float32)
            if kind == 3:
                own[s, :, cols] = t
            else:
                sbuf[p, :, cols] = t.astype(jnp.bfloat16)
                for r in pass_copies(kind, s, cols):
                    r.start()
            return 0

        lax.fori_loop(0, out // COLS, down_step, 0)

    for kind in range(1, 4):
        def body(s, _, kind=kind):
            run_pass(kind, s)
            return 0
        lax.fori_loop(0, 2, body, 0)

    def ag(owner, part, s, d, slot):
        at = row_of(owner, part, s * sub, sub)
        return remote(y_ref.at[at], y_ref.at[at], ag_send.at[s, d, slot], ag_recv.at[s, d, slot], (right, left)[d])

    for s in range(2):
        for c in pass_copies(2, s):
            c.wait_recv()
        for part in range(2):
            at = pl.ds(part * sub, sub)
            y_ref[row_of(me, part, s * sub, sub), :] = (
                own[s, at] + rbuf[2, s, at].astype(jnp.float32)).astype(jnp.bfloat16)
        for i in range(2):
            for d in range(2):
                q = i if d == 0 else 1 - i
                ag(me, q, s, d, q).start()

    def forward(s, d):
        return ag(left if d == 0 else right, d, s, d, 2)

    for s in range(2):
        for d in range(2):
            ag(me, d, s, d, d).wait_recv()
            forward(s, d).start()
    for s in range(2):
        for d in range(2):
            ag(me, 1 - d, s, d, 1 - d).wait_recv()
            forward(s, d).wait_recv()
    for q in range(MINI):
        for c in mini_copies(q):
            c.wait_send()
    for s in range(2):
        for kind in range(1, 3):
            for c in pass_copies(kind, s):
                c.wait_send()
        for d in range(2):
            for q in range(2):
                ag(me, q, s, d, q).wait_send()
            forward(s, d).wait_send()


def solution(mesh):
    n = mesh.shape["tp"]
    assert n == 4

    def step(x, w_gate, w_up, w_down):
        rows, depth = x.shape
        width, out = w_down.shape
        half = rows // n // 2
        bf16, f32 = jnp.bfloat16, jnp.float32
        any_ = pl.BlockSpec(memory_space=pl.ANY)
        dma = pltpu.SemaphoreType.DMA
        return pl.pallas_call(
            kernel,
            out_shape=pltpu.VMEM((rows, out), bf16),
            in_specs=[any_] * 4,
            out_specs=pl.BlockSpec(memory_space=pltpu.VMEM),
            scratch_shapes=[
                pltpu.VMEM((2, 2 * half // MINI, depth), bf16),
                pltpu.VMEM((2, half, depth), bf16),
                pltpu.VMEM((depth, width), bf16),
                pltpu.VMEM((depth, width), bf16),
                pltpu.VMEM((width, out), bf16),
                pltpu.VMEM((half, width), bf16),
                pltpu.VMEM((6, half, out), bf16),
                pltpu.VMEM((3, 2, half, out), bf16),
                pltpu.VMEM((2, half, out), f32),
                dma((2, 2)),
                dma((2, 2)),
                dma((len(UP), 2)),
                dma((len(DOWN),)),
                dma((MINI, 2)),
                dma((MINI, 2)),
                dma((6, 2)),
                dma((6, 2)),
                dma((2, 2, 3)),
                dma((2, 2, 3)),
            ],
            compiler_params=pltpu.CompilerParams(
                collective_id=0, has_side_effects=True, vmem_limit_bytes=52 * 2**20
            ),
            cost_estimate=pl.CostEstimate(
                flops=6 * rows * depth * width, bytes_accessed=2 * (2 * rows * depth + 3 * depth * width),
                transcendentals=rows * width),
            name="mlp_block",
        )(x, w_gate, w_up, w_down)

    return jax.shard_map(
        step,
        mesh=mesh,
        in_specs=(P("dp", None), P(None, "tp"), P(None, "tp"), P("tp", None)),
        out_specs=P("dp", None),
        check_vma=False,
    )
```

```python
import jax
import jax.numpy as jnp
from jax import lax
from jax.experimental import pallas as pl
from jax.experimental.pallas import tpu as pltpu
from jax.sharding import PartitionSpec as P

COLS = 512
UP = (1024, 512, 512)
DOWN = (512, 512, 512, 512)

MINI = 4
MINI_SEND = 1024
PASS_SEND = 512


def kernel(x_ref, wg_ref, wu_ref, wd_ref, y_ref, xmini, xbuf, wg, wu, wd, hid, sbuf, rbuf, own,
           xm_sem, x_sem, w_sem, d_sem, ms_sem, mr_sem, send_sem, recv_sem, ag_send, ag_recv):
    n = 4
    me = lax.axis_index("tp")
    right, left = lax.rem(me + 1, n), lax.rem(me + n - 1, n)
    rows = x_ref.shape[0]
    width, out = wd_ref.shape
    chunk = rows // n
    half = chunk // 2
    sub = half // 2
    mini = half // MINI

    def row_of(owner, part, at, size):
        return pl.ds(pl.multiple_of(lax.rem(owner, n) * chunk + part * half + at, size), size)

    def remote(src, dst, ssem, rsem, to):
        return pltpu.make_async_remote_copy(
            src_ref=src, dst_ref=dst, send_sem=ssem, recv_sem=rsem,
            device_id={"tp": to}, device_id_type=pl.DeviceIdType.MESH)

    def x_pair(kind, at, size, buf, sem):
        r = row_of(me + (4 - kind) // 2, lax.rem(kind + 1, 2), at, size)
        l = row_of(me + 2 + (kind + 1) // 2, lax.rem(kind, 2), at, size)
        return (
            pltpu.make_async_copy(x_ref.at[r], buf.at[pl.ds(0, size)], sem.at[0]),
            pltpu.make_async_copy(x_ref.at[l], buf.at[pl.ds(size, size)], sem.at[1]),
        )

    def x_mini(q):
        slot = lax.rem(q, 2)
        return x_pair(0, q * mini, mini, xmini.at[slot], xm_sem.at[slot])

    def x_pass(p):
        slot = lax.rem(p, 2)
        return x_pair(p // 2, slot * sub, sub, xbuf.at[slot], x_sem.at[slot])

    def w_copies(c):
        cols = pl.ds(sum(UP[:c]), UP[c])
        return (
            pltpu.make_async_copy(wg_ref.at[:, cols], wg.at[:, cols], w_sem.at[c, 0]),
            pltpu.make_async_copy(wu_ref.at[:, cols], wu.at[:, cols], w_sem.at[c, 1]),
        )

    def d_copy(c):
        cols = pl.ds(sum(DOWN[:c]), DOWN[c])
        return pltpu.make_async_copy(wd_ref.at[:, cols], wd.at[:, cols], d_sem.at[c])

    def mini_rows(q, d):
        return pl.ds(pl.multiple_of(lax.rem(q, 2) * mini + d * sub, mini), mini)

    def mini_copies(q, cols=slice(None)):
        s = q // 2
        return tuple(
            remote(sbuf.at[s, mini_rows(q, d), cols], rbuf.at[0, s, mini_rows(q, d), cols],
                   ms_sem.at[q, d], mr_sem.at[q, d], (right, left)[d])
            for d in range(2))

    def pass_copies(kind, s, cols=slice(None)):
        p = 2 * kind + s
        return tuple(
            remote(sbuf.at[p, pl.ds(d * sub, sub), cols],
                   rbuf.at[kind, s, pl.ds((1 - d if kind == 2 else d) * sub, sub), cols],
                   send_sem.at[p, d], recv_sem.at[p, d], (right, left)[d])
            for d in range(2))

    def gate_up(xv, cols):
        m = xv.shape[0]
        g = jnp.dot(xv, wg[:, cols], preferred_element_type=jnp.float32)
        u = jnp.dot(xv, wu[:, cols], preferred_element_type=jnp.float32)
        hid[pl.ds(0, m), cols] = (jax.nn.silu(g) * u).astype(jnp.bfloat16)

    def down(m, cols):
        return jnp.dot(hid[pl.ds(0, m)], wd[:, cols], preferred_element_type=jnp.float32)

    def step_cols(c):
        return pl.ds(pl.multiple_of(c * COLS, COLS), COLS)

    barrier = pltpu.get_barrier_semaphore()
    for to in (left, right):
        pl.semaphore_signal(barrier, inc=1, device_id={"tp": to}, device_id_type=pl.DeviceIdType.MESH)

    for c in x_mini(0):
        c.start()
    weights = [w_copies(c) for c in range(len(UP))] + [(d_copy(c),) for c in range(len(DOWN))]

    for i, group in enumerate(weights):
        for w in group:
            w.start(priority=0 if i < len(UP) else 1)
    for c in x_mini(1):
        c.start(priority=1)

    def store_mini(q, cols):
        t = down(2 * mini, cols).astype(jnp.bfloat16)
        for d in range(2):
            sbuf[q // 2, mini_rows(q, d), cols] = t[d * mini:(d + 1) * mini]

    for c in x_mini(0):
        c.wait()
    for c in range(len(UP)):
        for w in w_copies(c):
            w.wait()
        gate_up(xmini[0], pl.ds(sum(UP[:c]), UP[c]))
    pl.semaphore_wait(barrier, 2)
    for c in range(len(DOWN)):
        d_copy(c).wait()
        cols = pl.ds(sum(DOWN[:c]), DOWN[c])
        store_mini(0, cols)
        for r in mini_copies(0, cols):
            r.start()

    def mini_pass(q, _):
        for c in x_mini(q):
            c.wait()

        @pl.when(q < MINI - 1)
        def _():
            for c in x_mini(q + 1):
                c.start()

        @pl.when(q == MINI - 1)
        def _():
            for c in x_pass(2):
                c.start()

        slot = lax.rem(q, 2)

        def up_step(c, _):
            gate_up(xmini[slot], step_cols(c))
            return 0

        lax.fori_loop(0, width // COLS, up_step, 0)

        def down_steps(b, _):
            def down_step(c, _):
                store_mini(q, step_cols(c))
                return 0

            each = MINI_SEND // COLS
            lax.fori_loop(b * each, (b + 1) * each, down_step, 0)
            for r in mini_copies(q, pl.ds(pl.multiple_of(b * MINI_SEND, MINI_SEND), MINI_SEND)):
                r.start()
            return 0

        lax.fori_loop(0, out // MINI_SEND, down_steps, 0)
        return 0

    lax.fori_loop(1, MINI, mini_pass, 0)

    def run_pass(kind, s):
        p = 2 * kind + s
        for c in x_pass(p):
            c.wait()

        @pl.when(p < 7)
        def _():
            for c in x_pass(p + 1):
                c.start()

        def up_step(c, _):
            gate_up(xbuf[s], step_cols(c))
            return 0

        lax.fori_loop(0, width // COLS, up_step, 0)

        if kind == 2:
            for j in range(MINI // 2):
                for c in mini_copies(s * (MINI // 2) + j):
                    c.wait_recv()
        if kind == 3:
            for c in pass_copies(1, s):
                c.wait_recv()

        def down_step(c, _):
            cols = step_cols(c)
            t = down(2 * sub, cols)
            if kind >= 2:
                t = t + rbuf[kind - 2, s, :, cols].astype(jnp.float32)
            if kind == 3:
                own[s, :, cols] = t
            else:
                sbuf[p, :, cols] = t.astype(jnp.bfloat16)
            return 0

        send = (0, PASS_SEND, out, out)[kind]

        def down_steps(b, _):
            each = send // COLS
            lax.fori_loop(b * each, (b + 1) * each, down_step, 0)
            if kind < 3:
                for r in pass_copies(kind, s, pl.ds(pl.multiple_of(b * send, send), send)):
                    r.start()
            return 0

        lax.fori_loop(0, out // send, down_steps, 0)

    for kind in range(1, 4):
        def body(s, _, kind=kind):
            run_pass(kind, s)
            return 0
        lax.fori_loop(0, 2, body, 0)

    def ag(owner, part, s, d, slot):
        at = row_of(owner, part, s * sub, sub)
        return remote(y_ref.at[at], y_ref.at[at], ag_send.at[s, d, slot], ag_recv.at[s, d, slot], (right, left)[d])

    for s in range(2):
        for c in pass_copies(2, s):
            c.wait_recv()
        for part in range(2):
            at = pl.ds(part * sub, sub)
            y_ref[row_of(me, part, s * sub, sub), :] = (
                own[s, at] + rbuf[2, s, at].astype(jnp.float32)).astype(jnp.bfloat16)
        for i in range(2):
            for d in range(2):
                q = i if d == 0 else 1 - i
                ag(me, q, s, d, q).start()

    def forward(s, d):
        return ag(left if d == 0 else right, d, s, d, 2)

    for s in range(2):
        for d in range(2):
            ag(me, d, s, d, d).wait_recv()
            forward(s, d).start()
    for s in range(2):
        for d in range(2):
            ag(me, 1 - d, s, d, 1 - d).wait_recv()
            forward(s, d).wait_recv()
    for q in range(MINI):
        for c in mini_copies(q):
            c.wait_send()
    for s in range(2):
        for kind in range(1, 3):
            for c in pass_copies(kind, s):
                c.wait_send()
        for d in range(2):
            for q in range(2):
                ag(me, q, s, d, q).wait_send()
            forward(s, d).wait_send()


def solution(mesh):
    n = mesh.shape["tp"]
    assert n == 4

    def step(x, w_gate, w_up, w_down):
        rows, depth = x.shape
        width, out = w_down.shape
        half = rows // n // 2
        bf16, f32 = jnp.bfloat16, jnp.float32
        any_ = pl.BlockSpec(memory_space=pl.ANY)
        dma = pltpu.SemaphoreType.DMA
        return pl.pallas_call(
            kernel,
            out_shape=pltpu.VMEM((rows, out), bf16),
            in_specs=[any_] * 4,
            out_specs=pl.BlockSpec(memory_space=pltpu.VMEM),
            scratch_shapes=[
                pltpu.VMEM((2, 2 * half // MINI, depth), bf16),
                pltpu.VMEM((2, half, depth), bf16),
                pltpu.VMEM((depth, width), bf16),
                pltpu.VMEM((depth, width), bf16),
                pltpu.VMEM((width, out), bf16),
                pltpu.VMEM((half, width), bf16),
                pltpu.VMEM((6, half, out), bf16),
                pltpu.VMEM((3, 2, half, out), bf16),
                pltpu.VMEM((2, half, out), f32),
                dma((2, 2)),
                dma((2, 2)),
                dma((len(UP), 2)),
                dma((len(DOWN),)),
                dma((MINI, 2)),
                dma((MINI, 2)),
                dma((6, 2)),
                dma((6, 2)),
                dma((2, 2, 3)),
                dma((2, 2, 3)),
            ],
            compiler_params=pltpu.CompilerParams(
                collective_id=0, has_side_effects=True, vmem_limit_bytes=52 * 2**20
            ),
            cost_estimate=pl.CostEstimate(
                flops=6 * rows * depth * width, bytes_accessed=2 * (2 * rows * depth + 3 * depth * width),
                transcendentals=rows * width),
            name="mlp_block",
        )(x, w_gate, w_up, w_down)

    return jax.shard_map(
        step,
        mesh=mesh,
        in_specs=(P("dp", None), P(None, "tp"), P(None, "tp"), P("tp", None)),
        out_specs=P("dp", None),
        check_vma=False,
    )
```

```python
import jax
import jax.numpy as jnp
from jax import lax
from jax.experimental import pallas as pl
from jax.experimental.pallas import tpu as pltpu
from jax.sharding import PartitionSpec as P

COLS = 512
WIDE = 1024
UP = (1024, 512, 512)
DOWN = (512, 512, 512, 512)

MINI = 4
MINI_SEND = 1024
PASS_SEND = 1024


def kernel(x_ref, wg_ref, wu_ref, wd_ref, y_ref, xmini, xbuf, wg, wu, wd, hid, sbuf, rbuf, own,
           xm_sem, x_sem, w_sem, d_sem, ms_sem, mr_sem, send_sem, recv_sem, ag_send, ag_recv):
    n = 4
    me = lax.axis_index("tp")
    right, left = lax.rem(me + 1, n), lax.rem(me + n - 1, n)
    rows = x_ref.shape[0]
    width, out = wd_ref.shape
    chunk = rows // n
    half = chunk // 2
    sub = half // 2
    mini = half // MINI

    def row_of(owner, part, at, size):
        return pl.ds(pl.multiple_of(lax.rem(owner, n) * chunk + part * half + at, size), size)

    def remote(src, dst, ssem, rsem, to):
        return pltpu.make_async_remote_copy(
            src_ref=src, dst_ref=dst, send_sem=ssem, recv_sem=rsem,
            device_id={"tp": to}, device_id_type=pl.DeviceIdType.MESH)

    def x_pair(kind, at, size, buf, sem):
        r = row_of(me + (4 - kind) // 2, lax.rem(kind + 1, 2), at, size)
        l = row_of(me + 2 + (kind + 1) // 2, lax.rem(kind, 2), at, size)
        return (
            pltpu.make_async_copy(x_ref.at[r], buf.at[pl.ds(0, size)], sem.at[0]),
            pltpu.make_async_copy(x_ref.at[l], buf.at[pl.ds(size, size)], sem.at[1]),
        )

    def x_mini(q):
        slot = lax.rem(q, 2)
        return x_pair(0, q * mini, mini, xmini.at[slot], xm_sem.at[slot])

    def x_pass(p):
        slot = lax.rem(p, 2)
        return x_pair(p // 2, slot * sub, sub, xbuf.at[slot], x_sem.at[slot])

    def w_copies(c):
        cols = pl.ds(sum(UP[:c]), UP[c])
        return (
            pltpu.make_async_copy(wg_ref.at[:, cols], wg.at[:, cols], w_sem.at[c, 0]),
            pltpu.make_async_copy(wu_ref.at[:, cols], wu.at[:, cols], w_sem.at[c, 1]),
        )

    def d_copy(c):
        cols = pl.ds(sum(DOWN[:c]), DOWN[c])
        return pltpu.make_async_copy(wd_ref.at[:, cols], wd.at[:, cols], d_sem.at[c])

    wide = width // WIDE

    def wide_cols(c):
        return pl.ds(pl.multiple_of(c * WIDE, WIDE), WIDE)

    def mini_rows(q, d):
        return pl.ds(pl.multiple_of(lax.rem(q, 2) * mini + d * sub, mini), mini)

    def mini_copies(q, cols=slice(None)):
        s = q // 2
        return tuple(
            remote(sbuf.at[s, mini_rows(q, d), cols], rbuf.at[0, s, mini_rows(q, d), cols],
                   ms_sem.at[q, d], mr_sem.at[q, d], (right, left)[d])
            for d in range(2))

    def pass_copies(kind, s, cols=slice(None)):
        p = 2 * kind + s
        return tuple(
            remote(sbuf.at[p, pl.ds(d * sub, sub), cols],
                   rbuf.at[kind, s, pl.ds((1 - d if kind == 2 else d) * sub, sub), cols],
                   send_sem.at[p, d], recv_sem.at[p, d], (right, left)[d])
            for d in range(2))

    def gate_up(xv, cols):
        m = xv.shape[0]
        g = jnp.dot(xv, wg[:, cols], preferred_element_type=jnp.float32)
        u = jnp.dot(xv, wu[:, cols], preferred_element_type=jnp.float32)
        hid[pl.ds(0, m), cols] = (jax.nn.silu(g) * u).astype(jnp.bfloat16)

    def down(m, cols):
        return jnp.dot(hid[pl.ds(0, m)], wd[:, cols], preferred_element_type=jnp.float32)

    def step_cols(c):
        return pl.ds(pl.multiple_of(c * COLS, COLS), COLS)

    barrier = pltpu.get_barrier_semaphore()
    for to in (left, right):
        pl.semaphore_signal(barrier, inc=1, device_id={"tp": to}, device_id_type=pl.DeviceIdType.MESH)

    for c in x_mini(0):
        c.start()
    weights = [w_copies(c) for c in range(len(UP))] + [(d_copy(c),) for c in range(len(DOWN))]

    for i, group in enumerate(weights):
        for w in group:
            w.start(priority=0 if i < len(UP) else 1)
    for c in x_mini(1):
        c.start(priority=1)

    def store_mini(q, cols):
        t = down(2 * mini, cols).astype(jnp.bfloat16)
        for d in range(2):
            sbuf[q // 2, mini_rows(q, d), cols] = t[d * mini:(d + 1) * mini]

    for c in x_mini(0):
        c.wait()
    for c in range(len(UP)):
        for w in w_copies(c):
            w.wait()
        gate_up(xmini[0], pl.ds(sum(UP[:c]), UP[c]))
    pl.semaphore_wait(barrier, 2)
    for c in range(len(DOWN)):
        d_copy(c).wait()
        cols = pl.ds(sum(DOWN[:c]), DOWN[c])
        store_mini(0, cols)
        for r in mini_copies(0, cols):
            r.start()

    def mini_pass(q, _):
        for c in x_mini(q):
            c.wait()

        @pl.when(q < MINI - 1)
        def _():
            for c in x_mini(q + 1):
                c.start()

        @pl.when(q == MINI - 1)
        def _():
            for c in x_pass(2):
                c.start()

        slot = lax.rem(q, 2)

        def up_step(c, _):
            gate_up(xmini[slot], wide_cols(c))
            return 0

        lax.fori_loop(0, wide, up_step, 0)

        def down_step(b, _):
            cols = pl.ds(pl.multiple_of(b * MINI_SEND, MINI_SEND), MINI_SEND)
            store_mini(q, cols)
            for r in mini_copies(q, cols):
                r.start()
            return 0

        lax.fori_loop(0, out // MINI_SEND, down_step, 0)
        return 0

    lax.fori_loop(1, MINI, mini_pass, 0)

    def run_pass(kind, s):
        p = 2 * kind + s
        for c in x_pass(p):
            c.wait()

        @pl.when(p < 7)
        def _():
            for c in x_pass(p + 1):
                c.start()

        def up_step(c, _):
            gate_up(xbuf[s], wide_cols(c))
            return 0

        lax.fori_loop(0, wide, up_step, 0)

        if kind == 2:
            for j in range(MINI // 2):
                for c in mini_copies(s * (MINI // 2) + j):
                    c.wait_recv()
        if kind == 3:
            for c in pass_copies(1, s):
                c.wait_recv()

        cut = PASS_SEND if kind == 1 else WIDE

        def down_step(c, _):
            cols = pl.ds(pl.multiple_of(c * cut, cut), cut)
            t = down(2 * sub, cols)
            if kind >= 2:
                t = t + rbuf[kind - 2, s, :, cols].astype(jnp.float32)
            if kind == 3:
                own[s, :, cols] = t
            else:
                sbuf[p, :, cols] = t.astype(jnp.bfloat16)
            return 0

        send = (0, PASS_SEND, out, out)[kind]

        def down_steps(b, _):
            each = send // cut
            lax.fori_loop(b * each, (b + 1) * each, down_step, 0)
            if kind < 3:
                for r in pass_copies(kind, s, pl.ds(pl.multiple_of(b * send, send), send)):
                    r.start()
            return 0

        lax.fori_loop(0, out // send, down_steps, 0)

    for kind in range(1, 4):
        def body(s, _, kind=kind):
            run_pass(kind, s)
            return 0
        lax.fori_loop(0, 2, body, 0)

    def ag(owner, part, s, d, slot):
        at = row_of(owner, part, s * sub, sub)
        return remote(y_ref.at[at], y_ref.at[at], ag_send.at[s, d, slot], ag_recv.at[s, d, slot], (right, left)[d])

    for s in range(2):
        for c in pass_copies(2, s):
            c.wait_recv()
        for part in range(2):
            at = pl.ds(part * sub, sub)
            y_ref[row_of(me, part, s * sub, sub), :] = (
                own[s, at] + rbuf[2, s, at].astype(jnp.float32)).astype(jnp.bfloat16)
        for i in range(2):
            for d in range(2):
                q = i if d == 0 else 1 - i
                ag(me, q, s, d, q).start()

    def forward(s, d):
        return ag(left if d == 0 else right, d, s, d, 2)

    for s in range(2):
        for d in range(2):
            ag(me, d, s, d, d).wait_recv()
            forward(s, d).start()
    for s in range(2):
        for d in range(2):
            ag(me, 1 - d, s, d, 1 - d).wait_recv()
            forward(s, d).wait_recv()
    for q in range(MINI):
        for c in mini_copies(q):
            c.wait_send()
    for s in range(2):
        for kind in range(1, 3):
            for c in pass_copies(kind, s):
                c.wait_send()
        for d in range(2):
            for q in range(2):
                ag(me, q, s, d, q).wait_send()
            forward(s, d).wait_send()


def solution(mesh):
    n = mesh.shape["tp"]
    assert n == 4

    def step(x, w_gate, w_up, w_down):
        rows, depth = x.shape
        width, out = w_down.shape
        half = rows // n // 2
        bf16, f32 = jnp.bfloat16, jnp.float32
        any_ = pl.BlockSpec(memory_space=pl.ANY)
        dma = pltpu.SemaphoreType.DMA
        return pl.pallas_call(
            kernel,
            out_shape=pltpu.VMEM((rows, out), bf16),
            in_specs=[any_] * 4,
            out_specs=pl.BlockSpec(memory_space=pltpu.VMEM),
            scratch_shapes=[
                pltpu.VMEM((2, 2 * half // MINI, depth), bf16),
                pltpu.VMEM((2, half, depth), bf16),
                pltpu.VMEM((depth, width), bf16),
                pltpu.VMEM((depth, width), bf16),
                pltpu.VMEM((width, out), bf16),
                pltpu.VMEM((half, width), bf16),
                pltpu.VMEM((6, half, out), bf16),
                pltpu.VMEM((3, 2, half, out), bf16),
                pltpu.VMEM((2, half, out), f32),
                dma((2, 2)),
                dma((2, 2)),
                dma((len(UP), 2)),
                dma((len(DOWN),)),
                dma((MINI, 2)),
                dma((MINI, 2)),
                dma((6, 2)),
                dma((6, 2)),
                dma((2, 2, 3)),
                dma((2, 2, 3)),
            ],
            compiler_params=pltpu.CompilerParams(
                collective_id=0, has_side_effects=True, vmem_limit_bytes=52 * 2**20
            ),
            cost_estimate=pl.CostEstimate(
                flops=6 * rows * depth * width, bytes_accessed=2 * (2 * rows * depth + 3 * depth * width),
                transcendentals=rows * width),
            name="mlp_block",
        )(x, w_gate, w_up, w_down)

    return jax.shard_map(
        step,
        mesh=mesh,
        in_specs=(P("dp", None), P(None, "tp"), P(None, "tp"), P("tp", None)),
        out_specs=P("dp", None),
        check_vma=False,
    )
```
